8 devices in a mesh: dp: 1 (over z), tp: 8 (over x, y, core).
Axes of the slice: x: 2, y: 2, z: 1, core: 2. Of those that a mesh axis runs over, the one named last changes fastest.
Arguments:
- x: bfloat16 [2048, 9216], P('dp')
- gain: bfloat16 [9216], replicated
- wq: bfloat16 [9216, 9216], P(None, 'tp')
- wk: bfloat16 [9216, 9216], P(None, 'tp')
- wv: bfloat16 [9216, 9216], P(None, 'tp')
- wo: bfloat16 [9216, 9216], P('tp')
Outputs:
- output: bfloat16 [2048, 9216], P('dp')
All inputs are finite; a program needn't handle non-finite values.
Results may differ from the reference program's by a relative error of at most 0.012.
Values are sent between devices in bfloat16 or wider.
A program may use at most 2 GiB of HBM per device.

```python
import jax
import jax.numpy as jnp
from jax import lax

ROWS = 2048
D = 9216
HEADS = 72
KV_HEADS = 72
HEAD = 128
THETA = 10000


def setup_inputs(seed: int = 0, part: int = 0) -> dict:
    kx, kn, kq, kk, kv, ko = jax.random.split(jax.random.key(seed), 6)

    def weights(key, rows, columns):
        return jax.random.normal(key, (rows, columns), jnp.float32) * rows**-0.5

    drawn = {
        "x": jax.random.normal(jax.random.fold_in(kx, part), (ROWS, D), jnp.float32),
        "gain": 1 + 0.1 * jax.random.normal(kn, (D,), jnp.float32),
        "wq": 2 * weights(kq, D, HEADS * HEAD),
        "wk": 2 * weights(kk, D, KV_HEADS * HEAD),
        "wv": 4 * weights(kv, D, KV_HEADS * HEAD),
        "wo": weights(ko, HEADS * HEAD, D),
    }
    return {k: v.astype(jnp.bfloat16) for k, v in drawn.items()}


def normed(x, gain):
    wide = x.astype(jnp.float32)
    scale = lax.rsqrt(jnp.mean(wide * wide, -1, keepdims=True) + 1e-6)
    return (wide * scale * gain.astype(jnp.float32)).astype(jnp.bfloat16)


def turned(t, place, theta):
    half = t.shape[-1] // 2
    angle = place.astype(jnp.float32)[:, None] * theta ** (-jnp.arange(half, dtype=jnp.float32) / half)
    cos, sin = jnp.cos(angle)[:, None], jnp.sin(angle)[:, None]
    a, b = t[..., :half].astype(jnp.float32), t[..., half:].astype(jnp.float32)
    return jnp.concatenate([a * cos - b * sin, b * cos + a * sin], -1).astype(jnp.bfloat16)


def matmul(a, w):
    return jnp.dot(a, w, preferred_element_type=jnp.float32).astype(jnp.bfloat16)


def einsum(form, a, b):
    return jnp.einsum(form, a.astype(jnp.float32), b.astype(jnp.float32))


def attention(q, k, v):
    scores = einsum("tgsd,ugd->gstu", q, k) * q.shape[-1] ** -0.5
    token = jnp.arange(q.shape[0])
    scores = jnp.where(token[:, None] >= token, scores, -jnp.inf)
    weights = jax.nn.softmax(scores, -1).astype(jnp.bfloat16)
    return einsum("gstu,ugd->tgsd", weights, v).astype(jnp.bfloat16)


def reference(x, gain, wq, wk, wv, wo):
    a, place = normed(x, gain), jnp.arange(ROWS)
    q = turned(matmul(a, wq).reshape(ROWS, HEADS, HEAD), place, THETA).reshape(ROWS, KV_HEADS, -1, HEAD)
    k = turned(matmul(a, wk).reshape(ROWS, KV_HEADS, HEAD), place, THETA)
    v = matmul(a, wv).reshape(ROWS, KV_HEADS, HEAD)
    seen = attention(q, k, v).reshape(ROWS, HEADS * HEAD)
    return (x.astype(jnp.float32) + jnp.dot(seen, wo, preferred_element_type=jnp.float32)).astype(jnp.bfloat16)
```

```python
import functools

import jax
import jax.numpy as jnp
import numpy as np
from jax import lax
from jax.experimental import pallas as pl
from jax.experimental.pallas import tpu as pltpu
from jax.sharding import PartitionSpec as P

HEAD = 128
THETA = 10000
NEG = -1e30
HIDDEN = 2 * NEG
LOG2E = 1.4426950408889634
MESH = pl.DeviceIdType.MESH
BQ = 256
TILE = 256
RING = 4
S1, S2, G2, G1_OWN, G1_FAR, G0_OWN, G0_FAR, G0_NEAR, G0_DIAGONAL, COPIES = 4, 6, 7, 8, 9, 10, 11, 12, 13, 14


def dot(a, b, ca=1, cb=0):
    return lax.dot_general(a, b, (((ca,), (cb,)), ((), ())), preferred_element_type=jnp.float32)


def tables(tokens, half):
    angle = np.arange(tokens, dtype=np.float32)[:, None] * np.float32(THETA) ** (-np.arange(half, dtype=np.float32) / np.float32(half))
    cos, sin = np.cos(angle), np.sin(angle)
    return np.concatenate([cos, cos, -sin, sin], 1).astype(np.float32)


def kernel(x, gain, wq, wk, wv, wo, turn, y, r0, r1, r2, a, ring, kc, vc, q, wt, send0, send1, kept, send2, own, stage, top, mix, cs,
           ssem, rsem, ring_sem, wt_sem, x_sem, cs_sem, stage_sem, y_sem, *, rows, chunks):
    heads = q.shape[1] // HEAD
    depth, width = wq.shape[0], q.shape[1]
    half_depth = depth // 2
    tiles = (3 * heads + 1) // 2
    steps = 2 * tiles
    me = lax.axis_index("tp")
    core, yy, xx = me % 2, (me // 2) % 2, me // 4
    across_x, across_y = me + 4 - 8 * xx, me + 2 - 4 * yy
    mate = me + 1 - 2 * core
    near = across_x * (1 - core) + across_y * core
    far = across_y * (1 - core) + across_x * core
    diagonal = near + far - me
    mate_shift = mate - me
    scale = HEAD**-0.5 * LOG2E

    barrier = pltpu.get_barrier_semaphore()
    for d in (mate, near, far):
        pl.semaphore_signal(barrier, inc=1, device_id={"tp": d}, device_id_type=MESH)
    pl.semaphore_wait(barrier, 3)

    def span(c):
        return pl.ds(pl.multiple_of(c * rows, rows), rows)

    def cols(owner):
        return pl.ds(pl.multiple_of(owner * width, width), width)

    def remote(src, dst, c, t, dev):
        return pltpu.make_async_remote_copy(src_ref=src, dst_ref=dst, send_sem=ssem.at[c, t], recv_sem=rsem.at[c, t], device_id={"tp": dev},
                                            device_id_type=MESH)

    def s0(c, j):
        at = pl.ds(pl.multiple_of(j * width, width), width)
        return remote(send0.at[:, at], r0.at[span(c), at], c, j, mate)

    def s1(c, j):
        at = pl.ds(pl.multiple_of(j * width, width), width)
        return remote(send1.at[:, at], r1.at[span(c), at], c, S1 + j, near)

    def s2(c):
        return remote(send2, r2.at[span(c), :], c, S2, far)

    def gather_own(c, t, dev):
        return remote(own, y.at[span(c), cols(me)], c, t, dev)

    def gather(c, t, owner, dev):
        here = y.at[span(c), cols(owner)]
        return remote(here, here, c, t, dev)

    def keep_own(c):
        return pltpu.make_async_copy(own, y.at[span(c), cols(me)], y_sem)

    def load_stage(src, i):
        return pltpu.make_async_copy(src, stage.at[i], stage_sem.at[i])

    def by_rows(f, size=64):
        def body(i, _):
            f(pl.ds(pl.multiple_of(i * size, size), size))
        lax.fori_loop(0, rows // size, body, None)

    def after_near(c):
        s1(c, 0).wait()
        load = load_stage(r1.at[span(c), :width], 0)
        load.start()
        load.wait()

        def add(at):
            send2[at, :] = (kept[at, :width] + stage[0, at, :].astype(jnp.float32)).astype(jnp.bfloat16)
        by_rows(add)
        s2(c).start()

    def after_far(c):
        mine = pltpu.make_async_copy(x.at[span(c), cols(me)], own, y_sem)
        mine.start()
        s1(c, 1).wait()
        loads = [load_stage(r1.at[span(c), width:], 0), load_stage(r2.at[span(c), :], 1)]
        loads[0].start()
        s2(c).wait()
        loads[1].start()
        mine.wait()
        loads[0].wait()
        loads[1].wait()

        def add(at):
            total = kept[at, width:] + stage[0, at, :].astype(jnp.float32) + stage[1, at, :].astype(jnp.float32)
            own[at, :] = (own[at, :].astype(jnp.float32) + total).astype(jnp.bfloat16)
        by_rows(add)
        gather_own(c, G2, far).start()
        gather_own(c, G1_OWN, near).start()
        gather_own(c, G0_OWN, mate).start()
        keep_own(c).start()

    def after_g2(c):
        gather_own(c, G2, far).wait()
        gather(c, G1_FAR, far, near).start()
        gather(c, G0_FAR, far, mate).start()
        gather_own(c, G1_OWN, near).wait()
        gather(c, G0_NEAR, near, mate).start()
        gather_own(c, G0_OWN, mate).wait_send()
        keep_own(c).wait()

    def after_g1(c):
        gather(c, G1_FAR, far, near).wait()
        gather(c, G0_DIAGONAL, diagonal, mate).start()

    def finish(c):
        gather_own(c, G0_OWN, mate).wait_recv()
        gather(c, G0_FAR, far, mate).wait()
        gather(c, G0_NEAR, near, mate).wait()
        gather(c, G0_DIAGONAL, diagonal, mate).wait()

    def start_tile(n, slot):
        deep = pl.ds(pl.multiple_of((n % 2) * half_depth, half_depth), half_depth)
        for i in range(2):
            h = jnp.minimum(n // 2 * 2 + i, 3 * heads - 1)
            for m, w in enumerate((wq, wk, wv)):
                @pl.when(h // heads == m)
                def _():
                    at = pl.ds(pl.multiple_of((h % heads) * HEAD, HEAD), HEAD)
                    pltpu.make_async_copy(w.at[deep, at], ring.at[slot, :, i * HEAD : (i + 1) * HEAD], ring_sem.at[slot, i]).start()

    def wait_tile(slot):
        for i in range(2):
            pltpu.make_async_copy(wq.at[:half_depth, :HEAD], ring.at[slot, :, i * HEAD : (i + 1) * HEAD], ring_sem.at[slot, i]).wait()

    def load_x(c):
        return pltpu.make_async_copy(x.at[span(c), :], a, x_sem)

    def load_turn(c):
        return pltpu.make_async_copy(turn.at[span(c), :], cs, cs_sem)

    def load_wo(owner, slot):
        return pltpu.make_async_copy(wo.at[:, cols(owner)], wt.at[slot], wt_sem.at[slot])

    def piece(j):
        k = j % 4
        mine = jnp.where(k == 0, diagonal, jnp.where(k == 1, near, jnp.where(k == 2, far, me)))
        other = jnp.where(k == 0, diagonal, jnp.where(k == 1, far, jnp.where(k == 2, near, me))) + mate_shift
        return jnp.where(j < 4, other, mine)

    def norm():
        group, block = 16, 512

        def body(i, _):
            at = pl.ds(pl.multiple_of(i * group, group), group)
            total = jnp.zeros((group, block), jnp.float32)
            for k in range(0, depth, block):
                v = a[at, k : k + block].astype(jnp.float32)
                total += v * v
            s = lax.rsqrt(jnp.sum(total, -1, keepdims=True) * (1 / depth) + 1e-6)
            for k in range(0, depth, block):
                a[at, k : k + block] = (a[at, k : k + block].astype(jnp.float32) * s * gain[:, k : k + block]).astype(jnp.bfloat16)
        lax.fori_loop(0, rows // group, body, None)

    def project(c, action):
        def body(t, _):
            parts = []
            for k in range(2):
                n = 2 * t + k
                ahead = n + RING - 1

                @pl.when((ahead < steps) | (c < chunks - 1))
                def _():
                    start_tile(ahead % steps, ahead % RING)
                wait_tile(n % RING)
                parts.append(dot(a[:, k * half_depth : (k + 1) * half_depth], ring[n % RING]))
            got = (parts[0] + parts[1]).astype(jnp.bfloat16)
            for i in range(2):
                h = 2 * t + i
                v = got[:, i * HEAD : (i + 1) * HEAD]
                at = pl.ds(pl.multiple_of((h % heads) * HEAD, HEAD), HEAD)

                def turned():
                    wide = v.astype(jnp.float32)
                    return (wide * cs[:, :HEAD] + pltpu.roll(wide, HEAD // 2, 1) * cs[:, HEAD:]).astype(jnp.bfloat16)

                @pl.when(h < heads)
                def _():
                    q[:, at] = turned()

                @pl.when((h >= heads) & (h < 2 * heads))
                def _():
                    kc[span(c), at] = turned()

                @pl.when((h >= 2 * heads) & (h < 3 * heads))
                def _():
                    vc[h - 2 * heads, :HEAD, span(c)] = v.T
            action(t)
        lax.fori_loop(0, tiles, body, None)

    def attend(c):
        def queries(n, _):
            mine = pl.ds(pl.multiple_of(n * BQ, BQ), BQ)
            here = c * (rows // BQ) + n
            top[...] = jnp.full(top.shape, NEG, jnp.float32)
            mix[...] = jnp.zeros(mix.shape, jnp.float32)

            def block(j, masked):
                keys = pl.ds(pl.multiple_of(j * BQ, BQ), BQ)
                scores = [dot(kc[keys, h * HEAD : (h + 1) * HEAD], q[mine, h * HEAD : (h + 1) * HEAD], 1, 1) for h in range(heads)]
                weights, keeps = [], []
                for h, s in enumerate(scores):
                    if masked:
                        seen = lax.broadcasted_iota(jnp.int32, s.shape, 1) >= lax.broadcasted_iota(jnp.int32, s.shape, 0)
                        s = jnp.where(seen, s, HIDDEN)
                    old = top[h : h + 1, :]
                    new = jnp.maximum(old, s.max(axis=0, keepdims=True))
                    top[h : h + 1, :] = new
                    weights.append(jnp.exp2((s - new) * scale).astype(jnp.bfloat16))
                    keeps.append(jnp.exp2((old - new) * scale))
                for h, (p, keep) in enumerate(zip(weights, keeps)):
                    mix[h] = mix[h] * keep + dot(vc[h, :, keys], p)

            lax.fori_loop(0, here, lambda j, _: block(j, False), None)
            block(here, True)
            for h in range(heads):
                q[mine, h * HEAD : (h + 1) * HEAD] = (mix[h, :HEAD, :] * (1 / mix[h, HEAD : HEAD + 1, :])).T.astype(jnp.bfloat16)
        lax.fori_loop(0, rows // BQ, queries, None)

    def out_project(c):
        def body(j, _):
            @pl.when((j < 7) | (c < chunks - 1))
            def _():
                load_wo(piece((j + 1) % 8), (j + 1) % 2).start()

            @pl.when(j >= 4)
            def _():
                s0(c, j - 4).wait()
                load_stage(r0.at[span(c), pl.ds(pl.multiple_of((j - 4) * width, width), width)], 0).start()
            load_wo(0, j % 2).wait()
            term = dot(q[...], wt[j % 2])

            @pl.when(j < 4)
            def _():
                send0[:, pl.ds(pl.multiple_of(j * width, width), width)] = term.astype(jnp.bfloat16)
                s0(c, j).start()

            @pl.when(j >= 4)
            def _():
                load_stage(r0.at[span(c), :width], 0).wait()
                total = term + stage[0].astype(jnp.float32)

                @pl.when(j < 6)
                def _():
                    send1[:, pl.ds(pl.multiple_of((j - 4) * width, width), width)] = total.astype(jnp.bfloat16)
                    s1(c, j - 4).start()

                @pl.when(j >= 6)
                def _():
                    kept[:, pl.ds(pl.multiple_of((j - 6) * width, width), width)] = total
        lax.fori_loop(0, 8, body, None)

    load_x(0).start()
    load_turn(0).start()
    for n in range(RING - 1):
        start_tile(jnp.int32(n), n)
    load_wo(piece(0), 0).start()
    vc[:, HEAD:, :] = jnp.ones((heads, vc.shape[1] - HEAD, vc.shape[2]), jnp.bfloat16)

    def chunk(c, _):
        load_x(c).wait()
        norm()
        load_turn(c).wait()

        def action(t):
            for when, step, lag in ((2, after_near, 1), (5, after_g1, 2), (11, after_far, 1)):
                @pl.when((t == when) & (c >= lag))
                def _():
                    step(c - lag)
        project(c, action)

        @pl.when(c < chunks - 1)
        def _():
            load_x(c + 1).start()
            load_turn(c + 1).start()
        attend(c)
        out_project(c)

        @pl.when(c >= 1)
        def _():
            after_g2(c - 1)
    lax.fori_loop(0, chunks, chunk, None)

    last = chunks - 1
    after_near(last)
    after_g1(last - 1)
    after_far(last)
    after_g2(last)
    after_g1(last)
    lax.fori_loop(0, chunks, lambda c, _: finish(c), None)


def solution(mesh):
    def step(x, gain, wq, wk, wv, wo):
        tokens, depth = x.shape
        width = wq.shape[1]
        heads = width // HEAD
        chunks = 4
        rows = tokens // chunks
        anywhere = pl.BlockSpec(memory_space=pl.ANY)
        vmem = pl.BlockSpec(memory_space=pltpu.VMEM)
        bf16, f32 = jnp.bfloat16, jnp.float32
        return pl.pallas_call(
            functools.partial(kernel, rows=rows, chunks=chunks),
            out_shape=[jax.ShapeDtypeStruct((tokens, n), bf16) for n in (depth, 4 * width, 2 * width, width)],
            in_specs=[anywhere, vmem] + [anywhere] * 5,
            out_specs=[anywhere] * 4,
            scratch_shapes=[
                pltpu.VMEM((rows, depth), bf16),
                pltpu.VMEM((RING, depth // 2, TILE), bf16),
                pltpu.VMEM((tokens, width), bf16),
                pltpu.VMEM((heads, HEAD + 16, tokens), bf16),
                pltpu.VMEM((rows, width), bf16),
                pltpu.VMEM((2, width, width), bf16),
                pltpu.VMEM((rows, 4 * width), bf16),
                pltpu.VMEM((rows, 2 * width), bf16),
                pltpu.VMEM((rows, 2 * width), f32),
                pltpu.VMEM((rows, width), bf16),
                pltpu.VMEM((rows, width), bf16),
                pltpu.VMEM((2, rows, width), bf16),
                pltpu.VMEM((heads, BQ), f32),
                pltpu.VMEM((heads, HEAD + 16, BQ), f32),
                pltpu.VMEM((rows, 2 * HEAD), f32),
                pltpu.SemaphoreType.DMA((chunks, COPIES)),
                pltpu.SemaphoreType.DMA((chunks, COPIES)),
                pltpu.SemaphoreType.DMA((RING, 2)),
                pltpu.SemaphoreType.DMA((2,)),
                pltpu.SemaphoreType.DMA,
                pltpu.SemaphoreType.DMA,
                pltpu.SemaphoreType.DMA((2,)),
                pltpu.SemaphoreType.DMA,
            ],
            compiler_params=pltpu.CompilerParams(collective_id=0, has_side_effects=True, vmem_limit_bytes=67043328),
            name="layer",
        )(x, gain.astype(f32)[None], wq, wk, wv, wo, jnp.asarray(tables(tokens, HEAD // 2)))[0]

    tokens, columns = P("dp", None), P(None, "tp")
    return jax.shard_map(
        step,
        mesh=mesh,
        in_specs=(tokens, P(None), columns, columns, columns, P("tp", None)),
        out_specs=tokens,
        check_vma=False,
    )
```

```python
import jax
import jax.numpy as jnp
import numpy as np
from jax import lax
from jax.experimental import pallas as pl
from jax.experimental.pallas import tpu as pltpu
from jax.sharding import PartitionSpec as P

HEAD = 128
THETA = 10000
NEG = -1e30
HIDDEN = 2 * NEG
LOG2E = 1.4426950408889634
MESH = pl.DeviceIdType.MESH
UNIT = 256
TILE = 256
SINGLE, PAIRS = 2, 3
UNITS = SINGLE + 2 * PAIRS
S1, S2, G2, G1_OWN, G1_FAR, G0_OWN, G0_FAR, G0_NEAR, G0_DIAGONAL, COPIES = 4, 6, 7, 8, 9, 10, 11, 12, 13, 14


def dot(a, b, ca=1, cb=0):
    return lax.dot_general(a, b, (((ca,), (cb,)), ((), ())), preferred_element_type=jnp.float32)


def table(tokens, half):
    angle = np.arange(tokens, dtype=np.float32)[:, None] * np.float32(THETA) ** (-np.arange(half, dtype=np.float32) / np.float32(half))
    return np.concatenate([np.cos(angle), np.sin(angle)], 1).astype(np.float32)


def kernel(x, gain, wq, wk, wv, wo, turn, y, a, ring, big, vc, wt, fresh, send0, send1, kept, send2, own, r0, r1, r2, top, mix, raw, cs,
           ssem, rsem, ring_sem, wt_sem, x_sem, cs_sem, y_sem):
    tokens, depth = x.shape
    width = wq.shape[1]
    heads = width // HEAD
    tiles = (3 * heads + 1) // 2
    me = lax.axis_index("tp")
    core, yy, xx = me % 2, (me // 2) % 2, me // 4
    across_x, across_y = me + 4 - 8 * xx, me + 2 - 4 * yy
    mate = me + 1 - 2 * core
    near = across_x * (1 - core) + across_y * core
    far = across_y * (1 - core) + across_x * core
    diagonal = near + far - me
    scale = HEAD**-0.5 * LOG2E
    q_row, v_row = tokens, tokens + 2 * UNIT

    barrier = pltpu.get_barrier_semaphore()
    for d in (mate, near, far):
        pl.semaphore_signal(barrier, inc=1, device_id={"tp": d}, device_id_type=MESH)
    pl.semaphore_wait(barrier, 3)

    def span(u, n=1):
        return pl.ds(pl.multiple_of(u * UNIT, UNIT), n * UNIT)

    def cols(owner):
        return pl.ds(pl.multiple_of(owner * width, width), width)

    def remote(src, dst, u, t, dev):
        return pltpu.make_async_remote_copy(src_ref=src, dst_ref=dst, send_sem=ssem.at[u, t], recv_sem=rsem.at[u, t], device_id={"tp": dev},
                                            device_id_type=MESH)

    def s0(u, j):
        return remote(send0.at[:, cols(j)], r0.at[u % 2, :, cols(j)], u, j, mate)

    def s1(u, j):
        return remote(send1.at[u % 2, :, cols(j)], r1.at[u % 2, :, cols(j)], u, S1 + j, near)

    def s2(u):
        return remote(send2.at[u % 2], r2.at[u % 2], u, S2, far)

    def gather_own(u, t, dev):
        return remote(own.at[u % 2], y.at[span(u), cols(me)], u, t, dev)

    def gather(u, t, owner, dev):
        here = y.at[span(u), cols(owner)]
        return remote(here, here, u, t, dev)

    def keep_own(u):
        return pltpu.make_async_copy(own.at[u % 2], y.at[span(u), cols(me)], y_sem.at[u % 2])

    def residual(u):
        return pltpu.make_async_copy(x.at[span(u), cols(me)], own.at[u % 2], y_sem.at[u % 2])

    def by_rows(f, size=64):
        def body(i, _):
            f(pl.ds(pl.multiple_of(i * size, size), size))
        lax.fori_loop(0, UNIT // size, body, None)

    def after_near(u):
        residual(u).start()
        s1(u, 0).wait()

        def add(at):
            send2[u % 2, at, :] = (kept[u % 2, at, :width] + r1[u % 2, at, :width].astype(jnp.float32)).astype(jnp.bfloat16)
        by_rows(add)
        s2(u).start()

    def after_far(u):
        s1(u, 1).wait()
        s2(u).wait()
        residual(u).wait()

        def add(at):
            total = kept[u % 2, at, width:] + r1[u % 2, at, width:].astype(jnp.float32) + r2[u % 2, at, :].astype(jnp.float32)
            own[u % 2, at, :] = (own[u % 2, at, :].astype(jnp.float32) + total).astype(jnp.bfloat16)
        by_rows(add)
        gather_own(u, G2, far).start()
        gather_own(u, G1_OWN, near).start()
        gather_own(u, G0_OWN, mate).start()
        keep_own(u).start()

    def after_g2(u):
        gather_own(u, G2, far).wait()
        gather(u, G1_FAR, far, near).start()
        gather(u, G0_FAR, far, mate).start()
        gather_own(u, G1_OWN, near).wait()
        gather(u, G0_NEAR, near, mate).start()
        gather_own(u, G0_OWN, mate).wait_send()
        keep_own(u).wait()

    def after_g1(u):
        gather(u, G1_FAR, far, near).wait()
        gather(u, G0_DIAGONAL, diagonal, mate).start()

    def finish(u):
        gather_own(u, G0_OWN, mate).wait_recv()
        gather(u, G0_FAR, far, mate).wait()
        gather(u, G0_NEAR, near, mate).wait()
        gather(u, G0_DIAGONAL, diagonal, mate).wait()

    def start_tile(t, slot):
        matrix, first = 2 * t // heads, 2 * t % heads
        halves = (slice(None, depth // 2), slice(depth // 2, None))
        ws = (wq, wk, wv)
        for m, w in enumerate(ws):
            @pl.when((matrix == m) & (first < heads - 1))
            def _():
                at = pl.ds(pl.multiple_of(first * HEAD, HEAD), TILE)
                for part in halves:
                    pltpu.make_async_copy(w.at[part, at], ring.at[slot, part, :], ring_sem.at[slot]).start()

            @pl.when((matrix == m) & (first == heads - 1))
            def _():
                then = ws[min(m + 1, 2)]
                at = (heads - 1) * HEAD if m == 2 else 0
                pltpu.make_async_copy(w.at[:, width - HEAD :], ring.at[slot, :, :HEAD], ring_sem.at[slot]).start()
                pltpu.make_async_copy(then.at[:, at : at + HEAD], ring.at[slot, :, HEAD:], ring_sem.at[slot]).start()

    def wait_tile(slot):
        pltpu.make_async_copy(wq.at[:, :TILE], ring.at[slot], ring_sem.at[slot]).wait()

    def load_x(u, n):
        return pltpu.make_async_copy(x.at[span(u, n), :], a.at[: n * UNIT, :], x_sem)

    def load_turn(u, n):
        return pltpu.make_async_copy(turn.at[span(u, n), :], raw.at[: n * UNIT, :], cs_sem)

    def load_wo(owner, slot):
        return pltpu.make_async_copy(wo.at[:, cols(owner)], wt.at[slot], wt_sem.at[slot])

    def piece(n):
        mine = jnp.where(n < 4, jnp.where(n == 2, diagonal, near), jnp.where(n == 6, far, me))
        other = jnp.where(n < 4, jnp.where(n == 0, diagonal, far), jnp.where(n == 4, near, me)) + mate - me
        return jnp.where(n % 4 < 2, other, mine)

    def norm(first, count):
        group, block = 16, 512
        for i in range(count // group):
            at = pl.ds(pl.multiple_of(first + i * group, group), group)
            total = jnp.zeros((group, block), jnp.float32)
            for k in range(0, depth, block):
                v = a[at, k : k + block].astype(jnp.float32)
                total += v * v
            s = lax.rsqrt(jnp.sum(total, -1, keepdims=True) * (1 / depth) + 1e-6)
            for k in range(0, depth, block):
                a[at, k : k + block] = (a[at, k : k + block].astype(jnp.float32) * s * gain[:, k : k + block]).astype(jnp.bfloat16)

    def project(u, n, last, action):
        rows = n * UNIT
        load_turn(u, n).wait()
        t, r = raw[:rows, :], pltpu.roll(raw[:rows, :], HEAD // 2, 1)
        low = lax.broadcasted_iota(jnp.int32, t.shape, 1) < HEAD // 2
        cs[0, :rows, :HEAD] = jnp.where(low, t, r)
        cs[0, :rows, HEAD:] = jnp.where(low, -r, t)

        def store(t, count):
            for i in range(count):
                h = jnp.maximum(2 * t + i, 0)
                m = h // heads
                row = jnp.where(m == 0, q_row, jnp.where(m == 1, u * UNIT, v_row))
                which = jnp.where(m == 2, 1, 0)
                wide = fresh[t % 2, :rows, i * HEAD : (i + 1) * HEAD].astype(jnp.float32)
                turned = wide * cs[which, :rows, :HEAD] + pltpu.roll(wide, HEAD // 2, 1) * cs[which, :rows, HEAD:]
                big[pl.ds(pl.multiple_of(row, UNIT), rows), pl.ds(pl.multiple_of((h % heads) * HEAD, HEAD), HEAD)] = turned.astype(jnp.bfloat16)

        def body(t, _):
            @pl.when((t < tiles - 1) | jnp.logical_not(last))
            def _():
                start_tile((t + 1) % tiles, (t + 1) % 2)
            action(t)
            wait_tile(t % 2)
            fresh[t % 2, :rows, :] = dot(a[:rows, :], ring[t % 2]).astype(jnp.bfloat16)
            store(t + 1 - 2, 2)
        lax.fori_loop(0, tiles, body, None)
        store(tiles - 1, 1)
        for h in range(heads):
            vc[h, :HEAD, span(u, n)] = big[v_row : v_row + rows, h * HEAD : (h + 1) * HEAD].T

    def attend(u, mine):
        top[...] = jnp.full(top.shape, NEG, jnp.float32)
        mix[...] = jnp.zeros(mix.shape, jnp.float32)

        def block(j, masked):
            scores = [dot(big[span(j), h * HEAD : (h + 1) * HEAD], big[mine, h * HEAD : (h + 1) * HEAD], 1, 1) for h in range(heads)]
            weights, keeps = [], []
            for h, s in enumerate(scores):
                if masked:
                    seen = lax.broadcasted_iota(jnp.int32, s.shape, 1) >= lax.broadcasted_iota(jnp.int32, s.shape, 0)
                    s = jnp.where(seen, s, HIDDEN)
                old = top[h : h + 1, :]
                new = jnp.maximum(old, s.max(axis=0, keepdims=True))
                top[h : h + 1, :] = new
                weights.append(jnp.exp2((s - new) * scale).astype(jnp.bfloat16))
                keeps.append(jnp.exp2((old - new) * scale))
            for h, (p, keep) in enumerate(zip(weights, keeps)):
                mix[h] = mix[h] * keep + dot(vc[h, :, span(j)], p)

        lax.fori_loop(0, u, lambda j, _: block(j, False), None)
        block(u, True)
        for h in range(heads):
            big[mine, h * HEAD : (h + 1) * HEAD] = (mix[h, :HEAD, :] * (1 / mix[h, HEAD : HEAD + 1, :])).T.astype(jnp.bfloat16)

    def out_project(u, mine, last, ahead, action):
        def step(n):
            @pl.when((n < 7) | jnp.logical_not(last))
            def _():
                load_wo(piece((n + 1) % 8), (n + 1) % 2).start()
            action(n)

        def term(n):
            load_wo(0, n % 2).wait()
            norm(*ahead(n))
            return dot(big[mine, :], wt[n % 2])

        def others(first, j):
            def body(i, _):
                n = first + i
                step(n)
                send0[:, cols(j + i)] = term(n).astype(jnp.bfloat16)
                s0(u, j + i).start()
            lax.fori_loop(0, 2, body, None)

        def ours(first, j, put):
            def body(i, _):
                n = first + i
                step(n)
                s0(u, j + i).wait()
                put(i, term(n) + r0[u % 2, :, cols(j + i)].astype(jnp.float32))
            lax.fori_loop(0, 2, body, None)

        def send(i, total):
            send1[u % 2, :, cols(i)] = total.astype(jnp.bfloat16)
            s1(u, i).start()

        def keep(i, total):
            kept[u % 2, :, cols(i)] = total

        others(0, 0)
        ours(2, 0, send)
        others(4, 2)
        ours(6, 2, keep)

    def at_steps(*plan):
        def action(t):
            for when, guard, f, u in plan:
                @pl.when((t == when) & guard)
                def _():
                    f(u)
        return action

    yes = jnp.bool_(True)
    load_x(0, 1).start()
    load_turn(0, 1).start()
    start_tile(jnp.int32(0), 0)
    load_wo(piece(0), 0).start()
    cs[1, :, :HEAD] = jnp.ones((cs.shape[1], HEAD), jnp.float32)
    cs[1, :, HEAD:] = jnp.zeros((cs.shape[1], HEAD), jnp.float32)
    vc[:, HEAD:, :] = jnp.ones((heads, vc.shape[1] - HEAD, vc.shape[2]), jnp.bfloat16)
    load_x(0, 1).wait()

    def first_norm(i, _):
        norm(i * 32, 32)
    lax.fori_loop(0, UNIT // 32, first_norm, None)

    def single(u, _):
        later = u >= 1
        project(u, 1, False, at_steps((1, later, after_near, u - 1), (6, later, after_far, u - 1), (13, later, after_g2, u - 1)))

        @pl.when(u < SINGLE - 1)
        def _():
            load_x(u + 1, 1).start()
            load_turn(u + 1, 1).start()

        @pl.when(u == SINGLE - 1)
        def _():
            load_x(u + 1, 2).start()
            load_turn(u + 1, 2).start()
        mine = pl.ds(q_row, UNIT)
        attend(u, mine)

        @pl.when(u < SINGLE - 1)
        def _():
            load_x(u + 1, 1).wait()

        @pl.when(u == SINGLE - 1)
        def _():
            load_x(u + 1, 2).wait()
        out_project(u, mine, False, lambda n: (n * 64, 64), at_steps())
    lax.fori_loop(0, SINGLE, single, None)

    def pair(p, _):
        u = SINGLE + 2 * p
        first, last = p == 0, p == PAIRS - 1
        rest = jnp.logical_not(first)
        b, c = u - 2, u - 1
        project(u, 2, last, at_steps((1, first, after_near, c), (1, rest, after_far, b), (2, rest, after_near, c), (3, first, after_g1, b),
                                     (4, first, after_far, c), (11, rest, after_far, c), (11, rest, after_g2, b), (10, first, after_g2, c)))

        @pl.when(jnp.logical_not(last))
        def _():
            load_x(u + 2, 2).start()
            load_turn(u + 2, 2).start()

        def half(v, _):
            w = u + v
            mine = pl.ds(pl.multiple_of(q_row + v * UNIT, UNIT), UNIT)
            attend(w, mine)

            @pl.when((v == 0) & jnp.logical_not(last))
            def _():
                load_x(u + 2, 2).wait()
            out_project(w, mine, last & (v == 1), lambda n: ((v * 8 + n) * 32, 32),
                        at_steps((3, rest & (v == 0), after_g1, b), (3, first & (v == 0), after_g1, c), (5, rest & (v == 0), after_g2, c),
                                 (2, v == 1, after_near, u), (4, rest & (v == 1), after_g1, c)))
        lax.fori_loop(0, 2, half, None)
    lax.fori_loop(0, PAIRS, pair, None)

    b, c = UNITS - 2, UNITS - 1
    after_near(c)
    after_far(b)
    after_g2(b)
    after_far(c)
    after_g1(b)
    after_g2(c)
    after_g1(c)
    lax.fori_loop(0, UNITS, lambda u, _: finish(u), None)


def solution(mesh):
    def step(x, gain, wq, wk, wv, wo):
        tokens, depth = x.shape
        width = wq.shape[1]
        heads = width // HEAD
        anywhere = pl.BlockSpec(memory_space=pl.ANY)
        vmem = pl.BlockSpec(memory_space=pltpu.VMEM)
        bf16, f32 = jnp.bfloat16, jnp.float32
        return pl.pallas_call(
            kernel,
            out_shape=jax.ShapeDtypeStruct((tokens, depth), bf16),
            in_specs=[anywhere, vmem] + [anywhere] * 5,
            out_specs=anywhere,
            scratch_shapes=[
                pltpu.VMEM((2 * UNIT, depth), bf16),
                pltpu.VMEM((2, depth, TILE), bf16),
                pltpu.VMEM((tokens + 4 * UNIT, width), bf16),
                pltpu.VMEM((heads, HEAD + 16, tokens), bf16),
                pltpu.VMEM((2, width, width), bf16),
                pltpu.VMEM((2, 2 * UNIT, TILE), bf16),
                pltpu.VMEM((UNIT, 4 * width), bf16),
                pltpu.VMEM((2, UNIT, 2 * width), bf16),
                pltpu.VMEM((2, UNIT, 2 * width), f32),
                pltpu.VMEM((2, UNIT, width), bf16),
                pltpu.VMEM((2, UNIT, width), bf16),
                pltpu.VMEM((2, UNIT, 4 * width), bf16),
                pltpu.VMEM((2, UNIT, 2 * width), bf16),
                pltpu.VMEM((2, UNIT, width), bf16),
                pltpu.VMEM((heads, UNIT), f32),
                pltpu.VMEM((heads, HEAD + 16, UNIT), f32),
                pltpu.VMEM((2 * UNIT, HEAD), f32),
                pltpu.VMEM((2, 2 * UNIT, 2 * HEAD), f32),
                pltpu.SemaphoreType.DMA((UNITS, COPIES)),
                pltpu.SemaphoreType.DMA((UNITS, COPIES)),
                pltpu.SemaphoreType.DMA((2,)),
                pltpu.SemaphoreType.DMA((2,)),
                pltpu.SemaphoreType.DMA,
                pltpu.SemaphoreType.DMA,
                pltpu.SemaphoreType.DMA((2,)),
            ],
            compiler_params=pltpu.CompilerParams(collective_id=0, has_side_effects=True, vmem_limit_bytes=67043328),
            name="layer",
        )(x, gain.astype(f32)[None], wq, wk, wv, wo, jnp.asarray(table(tokens, HEAD // 2)))

    tokens, columns = P("dp", None), P(None, "tp")
    return jax.shard_map(
        step,
        mesh=mesh,
        in_specs=(tokens, P(None), columns, columns, columns, P("tp", None)),
        out_specs=tokens,
        check_vma=False,
    )
```

```python
import jax
import jax.numpy as jnp
import numpy as np
from jax import lax
from jax.experimental import pallas as pl
from jax.experimental.pallas import tpu as pltpu
from jax.sharding import PartitionSpec as P

HEAD = 128
THETA = 10000
NEG = -1e30
HIDDEN = 2 * NEG
LOG2E = 1.4426950408889634
MESH = pl.DeviceIdType.MESH
UNIT = 256
TILE = 256
SINGLE, PAIRS = 2, 3
UNITS = SINGLE + 2 * PAIRS
S1, S2, G2, G1_OWN, G1_FAR, G0_OWN, G0_FAR, G0_NEAR, G0_DIAGONAL, COPIES = 4, 6, 7, 8, 9, 10, 11, 12, 13, 14


def dot(a, b, ca=1, cb=0):
    return lax.dot_general(a, b, (((ca,), (cb,)), ((), ())), preferred_element_type=jnp.float32)


def table(tokens, half):
    angle = np.arange(tokens, dtype=np.float32)[:, None] * np.float32(THETA) ** (-np.arange(half, dtype=np.float32) / np.float32(half))
    return np.concatenate([np.cos(angle), np.sin(angle)], 1).astype(np.float32)


def kernel(x, gain, wq, wk, wv, wo, turn, y, a, ring, big, vc, wt, fresh, send0, send1, kept, send2, own, r0, r1, r2, top, mix, raw, cs,
           ssem, rsem, ring_sem, wt_sem, x_sem, cs_sem, y_sem, read_sem):
    tokens, depth = x.shape
    width = wq.shape[1]
    heads = width // HEAD
    tiles = (3 * heads + 1) // 2
    me = lax.axis_index("tp")
    core, yy, xx = me % 2, (me // 2) % 2, me // 4
    across_x, across_y = me + 4 - 8 * xx, me + 2 - 4 * yy
    mate = me + 1 - 2 * core
    near = across_x * (1 - core) + across_y * core
    far = across_y * (1 - core) + across_x * core
    diagonal = near + far - me
    scale = HEAD**-0.5 * LOG2E
    q_row, v_row = tokens, tokens + 2 * UNIT

    barrier = pltpu.get_barrier_semaphore()
    for d in (mate, near, far):
        pl.semaphore_signal(barrier, inc=1, device_id={"tp": d}, device_id_type=MESH)
    pl.semaphore_wait(barrier, 3)

    def span(u, n=1):
        return pl.ds(pl.multiple_of(u * UNIT, UNIT), n * UNIT)

    def cols(owner):
        return pl.ds(pl.multiple_of(owner * width, width), width)

    def remote(src, dst, u, t, dev):
        return pltpu.make_async_remote_copy(src_ref=src, dst_ref=dst, send_sem=ssem.at[u, t], recv_sem=rsem.at[u, t], device_id={"tp": dev},
                                            device_id_type=MESH)

    def s0(u, j):
        return remote(send0.at[pl.ds(pl.multiple_of(u % 2 * UNIT, UNIT), UNIT), cols(j % 2)], r0.at[u % 2, :, cols(j)], u, j, mate)

    def s1(u, j):
        return remote(send1.at[u % 2, :, cols(j)], r1.at[u % 2, :, cols(j)], u, S1 + j, near)

    def s2(u):
        return remote(send2.at[u % 2], r2.at[u % 2], u, S2, far)

    def gather_own(u, t, dev):
        return remote(own.at[u % 2], y.at[span(u), cols(me)], u, t, dev)

    def gather(u, t, owner, dev):
        here = y.at[span(u), cols(owner)]
        return remote(here, here, u, t, dev)

    def keep_own(u):
        return pltpu.make_async_copy(own.at[u % 2], y.at[span(u), cols(me)], y_sem.at[u % 2])

    def residual(u):
        return pltpu.make_async_copy(x.at[span(u), cols(me)], own.at[u % 2], y_sem.at[u % 2])

    def by_rows(f, size=64):
        def body(i, _):
            f(pl.ds(pl.multiple_of(i * size, size), size))
        lax.fori_loop(0, UNIT // size, body, None)

    def after_near(u):
        residual(u).start()
        s1(u, 0).wait()

        def add(at):
            send2[u % 2, at, :] = (kept[u % 2, at, :width] + r1[u % 2, at, :width].astype(jnp.float32)).astype(jnp.bfloat16)
        by_rows(add)
        s2(u).start()

    def after_far(u):
        s1(u, 1).wait()
        s2(u).wait()
        residual(u).wait()

        def add(at):
            total = kept[u % 2, at, width:] + r1[u % 2, at, width:].astype(jnp.float32) + r2[u % 2, at, :].astype(jnp.float32)
            own[u % 2, at, :] = (own[u % 2, at, :].astype(jnp.float32) + total).astype(jnp.bfloat16)
        by_rows(add)
        pl.semaphore_signal(read_sem, inc=1, device_id={"tp": near}, device_id_type=MESH)
        gather_own(u, G2, far).start()
        gather_own(u, G1_OWN, near).start()
        gather_own(u, G0_OWN, mate).start()
        keep_own(u).start()

    def after_g2(u):
        gather_own(u, G2, far).wait()
        gather(u, G1_FAR, far, near).start()
        gather(u, G0_FAR, far, mate).start()
        gather_own(u, G1_OWN, near).wait()
        gather(u, G0_NEAR, near, mate).start()
        gather_own(u, G0_OWN, mate).wait_send()
        keep_own(u).wait()

    def after_g1(u):
        gather(u, G1_FAR, far, near).wait()
        gather(u, G0_DIAGONAL, diagonal, mate).start()

    def finish(u):
        gather(u, G0_FAR, far, mate).wait()
        gather(u, G0_NEAR, near, mate).wait()
        gather(u, G0_DIAGONAL, diagonal, mate).wait()

    def start_tile(t, slot):
        matrix, first = 2 * t // heads, 2 * t % heads
        halves = (slice(None, depth // 2), slice(depth // 2, None))
        ws = (wq, wk, wv)
        for m, w in enumerate(ws):
            @pl.when((matrix == m) & (first < heads - 1))
            def _():
                at = pl.ds(pl.multiple_of(first * HEAD, HEAD), TILE)
                for part in halves:
                    pltpu.make_async_copy(w.at[part, at], ring.at[slot, part, :], ring_sem.at[slot]).start()

            @pl.when((matrix == m) & (first == heads - 1))
            def _():
                then = ws[min(m + 1, 2)]
                at = (heads - 1) * HEAD if m == 2 else 0
                pltpu.make_async_copy(w.at[:, width - HEAD :], ring.at[slot, :, :HEAD], ring_sem.at[slot]).start()
                pltpu.make_async_copy(then.at[:, at : at + HEAD], ring.at[slot, :, HEAD:], ring_sem.at[slot]).start()

    def wait_tile(slot):
        pltpu.make_async_copy(wq.at[:, :TILE], ring.at[slot], ring_sem.at[slot]).wait()

    def load_x(u, n):
        return pltpu.make_async_copy(x.at[span(u, n), :], a.at[: n * UNIT, :], x_sem)

    def load_turn(u, n):
        return pltpu.make_async_copy(turn.at[span(u, n), :], raw.at[: n * UNIT, :], cs_sem)

    def load_wo(owner, slot):
        return pltpu.make_async_copy(wo.at[:, cols(owner)], wt.at[slot], wt_sem.at[slot])

    def piece(n):
        mine = jnp.where(n < 4, jnp.where(n == 2, diagonal, near), jnp.where(n == 6, far, me))
        other = jnp.where(n < 4, jnp.where(n == 0, diagonal, far), jnp.where(n == 4, near, me)) + mate - me
        return jnp.where(n % 4 < 2, other, mine)

    def norm(first, count):
        group, block = 16, 512
        for i in range(count // group):
            at = pl.ds(pl.multiple_of(first + i * group, group), group)
            total = jnp.zeros((group, block), jnp.float32)
            for k in range(0, depth, block):
                v = a[at, k : k + block].astype(jnp.float32)
                total += v * v
            s = lax.rsqrt(jnp.sum(total, -1, keepdims=True) * (1 / depth) + 1e-6)
            for k in range(0, depth, block):
                a[at, k : k + block] = (a[at, k : k + block].astype(jnp.float32) * s * gain[:, k : k + block].astype(jnp.float32)).astype(jnp.bfloat16)

    def project(u, n, last, action):
        rows = n * UNIT
        load_turn(u, n).wait()
        t, r = raw[:rows, :], pltpu.roll(raw[:rows, :], HEAD // 2, 1)
        low = lax.broadcasted_iota(jnp.int32, t.shape, 1) < HEAD // 2
        cs[0, :rows, :HEAD] = jnp.where(low, t, r)
        cs[0, :rows, HEAD:] = jnp.where(low, -r, t)

        def store(t, count):
            for i in range(count):
                h = jnp.maximum(2 * t + i, 0)
                m = h // heads
                row = jnp.where(m == 0, q_row, jnp.where(m == 1, u * UNIT, v_row))
                which = jnp.where(m == 2, 1, 0)
                wide = fresh[t % 2, :rows, i * HEAD : (i + 1) * HEAD].astype(jnp.float32)
                turned = wide * cs[which, :rows, :HEAD] + pltpu.roll(wide, HEAD // 2, 1) * cs[which, :rows, HEAD:]
                big[pl.ds(pl.multiple_of(row, UNIT), rows), pl.ds(pl.multiple_of((h % heads) * HEAD, HEAD), HEAD)] = turned.astype(jnp.bfloat16)

        def body(t, _):
            @pl.when((t < tiles - 1) | jnp.logical_not(last))
            def _():
                start_tile((t + 1) % tiles, (t + 1) % 2)
            action(t)
            wait_tile(t % 2)
            store(t + 1 - 2, 2)
            fresh[t % 2, :rows, :] = dot(a[:rows, :], ring[t % 2]).astype(jnp.bfloat16)
        lax.fori_loop(0, tiles, body, None)
        store(tiles - 1, 1)
        for h in range(heads):
            vc[h, :HEAD, span(u, n)] = big[v_row : v_row + rows, h * HEAD : (h + 1) * HEAD].T

    def attend(u, mine):
        top[...] = jnp.full(top.shape, NEG, jnp.float32)
        mix[...] = jnp.zeros(mix.shape, jnp.float32)

        def block(j, masked):
            scores = [dot(big[span(j), h * HEAD : (h + 1) * HEAD], big[mine, h * HEAD : (h + 1) * HEAD], 1, 1) for h in range(heads)]
            weights, keeps = [], []
            for h, s in enumerate(scores):
                if masked:
                    seen = lax.broadcasted_iota(jnp.int32, s.shape, 1) >= lax.broadcasted_iota(jnp.int32, s.shape, 0)
                    s = jnp.where(seen, s, HIDDEN)
                old = top[h : h + 1, :]
                new = jnp.maximum(old, s.max(axis=0, keepdims=True))
                top[h : h + 1, :] = new
                weights.append(jnp.exp2((s - new) * scale).astype(jnp.bfloat16))
                keeps.append(jnp.exp2((old - new) * scale))
            for h, (p, keep) in enumerate(zip(weights, keeps)):
                mix[h] = mix[h] * keep + dot(vc[h, :, span(j)], p)

        lax.fori_loop(0, u, lambda j, _: block(j, False), None)
        block(u, True)
        for h in range(heads):
            big[mine, h * HEAD : (h + 1) * HEAD] = (mix[h, :HEAD, :] * (1 / mix[h, HEAD : HEAD + 1, :])).T.astype(jnp.bfloat16)

    def out_project(u, count, turn_no, last, ahead, action, ready):
        rows = count * UNIT
        at = pl.ds(pl.multiple_of(u % 2 * UNIT, UNIT), rows) if count == 1 else slice(None)

        def step(n):
            @pl.when((n < 6) | jnp.logical_not(last))
            def _():
                load_wo(piece((n + 2) % 8), (8 * turn_no + n + 2) % 3).start()
            action(n)

        def term(n):
            slot = (8 * turn_no + n) % 3
            load_wo(0, slot).wait()
            norm(*ahead(n))
            return dot(big[q_row : q_row + rows, :], wt[slot])

        def others(first, j):
            def body(i, _):
                n = first + i
                step(n)
                send0[at, cols(i)] = term(n).astype(jnp.bfloat16)
                for v in range(count):
                    s0(u + v, j + i).start()
            lax.fori_loop(0, 2, body, None)

        def ours(first, j, put):
            def body(i, _):
                n = first + i
                step(n)
                for v in range(count):
                    s0(u + v, j + i).wait()
                got = term(n)
                for v in range(count):
                    put(u + v, i, got[v * UNIT : (v + 1) * UNIT] + r0[(u + v) % 2, :, cols(j + i)].astype(jnp.float32))
                if put is send:
                    for v in range(count):
                        s1(u + v, i).start()
            lax.fori_loop(0, 2, body, None)

        def send(w, i, total):
            send1[w % 2, :, cols(i)] = total.astype(jnp.bfloat16)

        def keep(w, i, total):
            kept[w % 2, :, cols(i)] = total

        others(0, 0)
        ready()
        ours(2, 0, send)
        others(4, 2)
        ours(6, 2, keep)

    def at_steps(*plan):
        def action(t):
            for when, guard, f, u in plan:
                @pl.when((t == when) & guard)
                def _():
                    f(u)
        return action

    yes = jnp.bool_(True)
    load_x(0, 1).start()
    load_turn(0, 1).start()
    start_tile(jnp.int32(0), 0)
    load_wo(piece(0), 0).start()
    load_wo(piece(1), 1).start()
    cs[1, :, :HEAD] = jnp.ones((cs.shape[1], HEAD), jnp.float32)
    cs[1, :, HEAD:] = jnp.zeros((cs.shape[1], HEAD), jnp.float32)
    vc[:, HEAD:, :] = jnp.ones((heads, vc.shape[1] - HEAD, vc.shape[2]), jnp.bfloat16)
    load_x(0, 1).wait()

    def first_norm(i, _):
        norm(i * 32, 32)
    lax.fori_loop(0, UNIT // 32, first_norm, None)

    def single(u, _):
        later = u >= 1
        project(u, 1, False, at_steps((1, later, after_near, u - 1), (6, later, after_far, u - 1), (13, later, after_g2, u - 1)))

        @pl.when(u < SINGLE - 1)
        def _():
            load_x(u + 1, 1).start()
            load_turn(u + 1, 1).start()

        @pl.when(u == SINGLE - 1)
        def _():
            load_x(u + 1, 2).start()
            load_turn(u + 1, 2).start()
        mine = pl.ds(q_row, UNIT)
        attend(u, mine)

        @pl.when(u < SINGLE - 1)
        def _():
            load_x(u + 1, 1).wait()

        @pl.when(u == SINGLE - 1)
        def _():
            load_x(u + 1, 2).wait()
        out_project(u, 1, u, False, lambda n: (n * 64, 64), at_steps(), lambda: None)
    lax.fori_loop(0, SINGLE, single, None)

    def pair(p, _):
        u = SINGLE + 2 * p
        first, last = p == 0, p == PAIRS - 1
        rest = jnp.logical_not(first)
        b, c = u - 2, u - 1
        project(u, 2, last, at_steps((2, first, after_near, c), (6, first, after_g1, b), (5, first, after_far, c), (13, first, after_g2, c),
                                     (0, rest, after_near, b), (4, rest, after_near, c), (12, p >= 2, after_g1, b - 2),
                                     (8, rest, after_far, b), (11, rest, after_far, c)))

        @pl.when(jnp.logical_not(last))
        def _():
            load_x(u + 2, 2).start()
            load_turn(u + 2, 2).start()

        def half(v, _):
            attend(u + v, pl.ds(pl.multiple_of(q_row + v * UNIT, UNIT), UNIT))
        lax.fori_loop(0, 2, half, None)

        @pl.when(jnp.logical_not(last))
        def _():
            load_x(u + 2, 2).wait()
        for w in (b, c):
            gather_own(w, G0_OWN, mate).wait_recv()
        out_project(u, 2, SINGLE + p, last, lambda n: (n * 64, 64), at_steps((2, first, after_g1, c), (0, rest, after_g2, b), (5, p >= 2, after_g1, c - 2), (7, rest, after_g2, c)),
                    lambda: pl.semaphore_wait(read_sem, 2))
    lax.fori_loop(0, PAIRS, pair, None)

    b, c = UNITS - 2, UNITS - 1
    after_near(b)
    after_near(c)
    after_far(b)
    after_g1(c - 2)
    after_g1(b - 2)
    after_far(c)
    after_g2(b)
    after_g2(c)
    after_g1(c)
    after_g1(b)
    pl.semaphore_wait(read_sem, 2)
    for w in (b, c):
        gather_own(w, G0_OWN, mate).wait_recv()
    lax.fori_loop(0, UNITS, lambda u, _: finish(u), None)


def solution(mesh):
    def step(x, gain, wq, wk, wv, wo):
        tokens, depth = x.shape
        width = wq.shape[1]
        heads = width // HEAD
        anywhere = pl.BlockSpec(memory_space=pl.ANY)
        vmem = pl.BlockSpec(memory_space=pltpu.VMEM)
        bf16, f32 = jnp.bfloat16, jnp.float32
        return pl.pallas_call(
            kernel,
            out_shape=jax.ShapeDtypeStruct((tokens, depth), bf16),
            in_specs=[anywhere, vmem] + [anywhere] * 5,
            out_specs=anywhere,
            scratch_shapes=[
                pltpu.VMEM((2 * UNIT, depth), bf16),
                pltpu.VMEM((2, depth, TILE), bf16),
                pltpu.VMEM((tokens + 4 * UNIT, width), bf16),
                pltpu.VMEM((heads, HEAD + 16, tokens), bf16),
                pltpu.VMEM((3, width, width), bf16),
                pltpu.VMEM((2, 2 * UNIT, TILE), bf16),
                pltpu.VMEM((2 * UNIT, 2 * width), bf16),
                pltpu.VMEM((2, UNIT, 2 * width), bf16),
                pltpu.VMEM((2, UNIT, 2 * width), f32),
                pltpu.VMEM((2, UNIT, width), bf16),
                pltpu.VMEM((2, UNIT, width), bf16),
                pltpu.VMEM((2, UNIT, 4 * width), bf16),
                pltpu.VMEM((2, UNIT, 2 * width), bf16),
                pltpu.VMEM((2, UNIT, width), bf16),
                pltpu.VMEM((heads, UNIT), f32),
                pltpu.VMEM((heads, HEAD + 16, UNIT), f32),
                pltpu.VMEM((2 * UNIT, HEAD), f32),
                pltpu.VMEM((2, 2 * UNIT, 2 * HEAD), f32),
                pltpu.SemaphoreType.DMA((UNITS, COPIES)),
                pltpu.SemaphoreType.DMA((UNITS, COPIES)),
                pltpu.SemaphoreType.DMA((2,)),
                pltpu.SemaphoreType.DMA((3,)),
                pltpu.SemaphoreType.DMA,
                pltpu.SemaphoreType.DMA,
                pltpu.SemaphoreType.DMA((2,)),
                pltpu.SemaphoreType.REGULAR,
            ],
            compiler_params=pltpu.CompilerParams(collective_id=0, has_side_effects=True, vmem_limit_bytes=67043328),
            name="layer",
        )(x, gain[None], wq, wk, wv, wo, jnp.asarray(table(tokens, HEAD // 2)))

    tokens, columns = P("dp", None), P(None, "tp")
    return jax.shard_map(
        step,
        mesh=mesh,
        in_specs=(tokens, P(None), columns, columns, columns, P("tp", None)),
        out_specs=tokens,
        check_vma=False,
    )
```

```python
import jax
import jax.numpy as jnp
import numpy as np
from jax import lax
from jax.experimental import pallas as pl
from jax.experimental.pallas import tpu as pltpu
from jax.sharding import PartitionSpec as P

HEAD = 128
THETA = 10000
NEG = -1e30
HIDDEN = 2 * NEG
LOG2E = 1.4426950408889634
MESH = pl.DeviceIdType.MESH
UNIT = 256
TILE = 256
PAIRS = 4
UNITS = 2 * PAIRS
S1, S2, G2, G1_OWN, G1_FAR, G0_OWN, G0_FAR, G0_NEAR, G0_DIAGONAL, COPIES = 4, 6, 7, 8, 9, 10, 11, 12, 13, 14


def dot(a, b, ca=1, cb=0):
    return lax.dot_general(a, b, (((ca,), (cb,)), ((), ())), preferred_element_type=jnp.float32)


def table(tokens, half):
    angle = np.arange(tokens, dtype=np.float32)[:, None] * np.float32(THETA) ** (-np.arange(half, dtype=np.float32) / np.float32(half))
    return np.concatenate([np.cos(angle), np.sin(angle)], 1).astype(np.float32)


def kernel(x, gain, wq, wk, wv, wo, turn, y, a, ring, big, vc, wt, fresh, send0, send1, kept, send2, own, r0, r1, r2, top, mix, raw, cs,
           ssem, rsem, ring_sem, wt_sem, x_sem, cs_sem, y_sem, read_sem, first_sem):
    tokens, depth = x.shape
    width = wq.shape[1]
    heads = width // HEAD
    tiles = (3 * heads + 1) // 2
    me = lax.axis_index("tp")
    core, yy, xx = me % 2, (me // 2) % 2, me // 4
    across_x, across_y = me + 4 - 8 * xx, me + 2 - 4 * yy
    mate = me + 1 - 2 * core
    near = across_x * (1 - core) + across_y * core
    far = across_y * (1 - core) + across_x * core
    diagonal = near + far - me
    scale = HEAD**-0.5 * LOG2E
    q_row, v_row = tokens, tokens + 2 * UNIT

    barrier = pltpu.get_barrier_semaphore()
    for d in (mate, near, far):
        pl.semaphore_signal(barrier, inc=1, device_id={"tp": d}, device_id_type=MESH)
    pl.semaphore_wait(barrier, 3)

    def span(u, n=1):
        return pl.ds(pl.multiple_of(u * UNIT, UNIT), n * UNIT)

    def cols(owner):
        return pl.ds(pl.multiple_of(owner * width, width), width)

    def remote(src, dst, u, t, dev):
        return pltpu.make_async_remote_copy(src_ref=src, dst_ref=dst, send_sem=ssem.at[u, t], recv_sem=rsem.at[u, t], device_id={"tp": dev},
                                            device_id_type=MESH)

    def s0(u, j):
        return remote(send0.at[pl.ds(pl.multiple_of(u % 2 * UNIT, UNIT), UNIT), cols(j % 2)], r0.at[u % 2, :, cols(j)], u, j, mate)

    def s1(u, j):
        return remote(send1.at[u % 2, :, cols(j)], r1.at[u % 2, :, cols(j)], u, S1 + j, near)

    def s2(u):
        return remote(send2.at[u % 2], r2.at[u % 2], u, S2, far)

    def gather_own(u, t, dev):
        return remote(own.at[u % 2], y.at[span(u), cols(me)], u, t, dev)

    def gather(u, t, owner, dev):
        here = y.at[span(u), cols(owner)]
        return remote(here, here, u, t, dev)

    def keep_own(u):
        return pltpu.make_async_copy(own.at[u % 2], y.at[span(u), cols(me)], y_sem.at[u % 2])

    def residual(u):
        return pltpu.make_async_copy(x.at[span(u), cols(me)], own.at[u % 2], y_sem.at[u % 2])

    def by_rows(f, size=64):
        def body(i, _):
            f(pl.ds(pl.multiple_of(i * size, size), size))
        lax.fori_loop(0, UNIT // size, body, None)

    def after_near(u):
        residual(u).start()
        s1(u, 0).wait()

        def add(at):
            send2[u % 2, at, :] = (kept[u % 2, at, :width] + r1[u % 2, at, :width].astype(jnp.float32)).astype(jnp.bfloat16)
        by_rows(add)
        s2(u).start()

    def after_far(u):
        s1(u, 1).wait()
        s2(u).wait()
        residual(u).wait()

        def add(at):
            total = kept[u % 2, at, width:] + r1[u % 2, at, width:].astype(jnp.float32) + r2[u % 2, at, :].astype(jnp.float32)
            own[u % 2, at, :] = (own[u % 2, at, :].astype(jnp.float32) + total).astype(jnp.bfloat16)
        by_rows(add)
        pl.semaphore_signal(read_sem, inc=1, device_id={"tp": near}, device_id_type=MESH)
        gather_own(u, G2, far).start()
        gather_own(u, G1_OWN, near).start()
        gather_own(u, G0_OWN, mate).start()
        keep_own(u).start()

    def after_g2(u):
        gather_own(u, G2, far).wait()
        gather(u, G1_FAR, far, near).start()
        gather(u, G0_FAR, far, mate).start()
        gather_own(u, G1_OWN, near).wait()
        gather(u, G0_NEAR, near, mate).start()
        gather_own(u, G0_OWN, mate).wait_send()
        keep_own(u).wait()

    def after_g1(u):
        gather(u, G1_FAR, far, near).wait()
        gather(u, G0_DIAGONAL, diagonal, mate).start()

    def finish(u):
        gather(u, G0_FAR, far, mate).wait()
        gather(u, G0_NEAR, near, mate).wait()
        gather(u, G0_DIAGONAL, diagonal, mate).wait()

    def start_tile(t, slot):
        matrix, first = 2 * t // heads, 2 * t % heads
        halves = (slice(None, depth // 2), slice(depth // 2, None))
        ws = (wq, wk, wv)
        for m, w in enumerate(ws):
            @pl.when((matrix == m) & (first < heads - 1))
            def _():
                at = pl.ds(pl.multiple_of(first * HEAD, HEAD), TILE)
                for part in halves:
                    pltpu.make_async_copy(w.at[part, at], ring.at[slot, part, :], ring_sem.at[slot]).start()

            @pl.when((matrix == m) & (first == heads - 1))
            def _():
                then = ws[min(m + 1, 2)]
                at = (heads - 1) * HEAD if m == 2 else 0
                pltpu.make_async_copy(w.at[:, width - HEAD :], ring.at[slot, :, :HEAD], ring_sem.at[slot]).start()
                pltpu.make_async_copy(then.at[:, at : at + HEAD], ring.at[slot, :, HEAD:], ring_sem.at[slot]).start()

    def wait_tile(slot):
        pltpu.make_async_copy(wq.at[:, :TILE], ring.at[slot], ring_sem.at[slot]).wait()

    def load_x(u, n):
        return pltpu.make_async_copy(x.at[span(u, n), :], a.at[: n * UNIT, :], x_sem)

    def load_turn(u, n):
        return pltpu.make_async_copy(turn.at[span(u, n), :], raw.at[: n * UNIT, :], cs_sem)

    def load_wo(owner, slot):
        return pltpu.make_async_copy(wo.at[:, cols(owner)], wt.at[slot], wt_sem.at[slot])

    def piece(n):
        mine = jnp.where(n < 4, jnp.where(n == 2, diagonal, near), jnp.where(n == 6, far, me))
        other = jnp.where(n < 4, jnp.where(n == 0, diagonal, far), jnp.where(n == 4, near, me)) + mate - me
        return jnp.where(n % 4 < 2, other, mine)

    def norm(first, count):
        group, block = 16, 512
        for i in range(count // group):
            at = pl.ds(pl.multiple_of(first + i * group, group), group)
            total = jnp.zeros((group, block), jnp.float32)
            for k in range(0, depth, block):
                v = a[at, k : k + block].astype(jnp.float32)
                total += v * v
            s = lax.rsqrt(jnp.sum(total, -1, keepdims=True) * (1 / depth) + 1e-6)
            for k in range(0, depth, block):
                a[at, k : k + block] = (a[at, k : k + block].astype(jnp.float32) * s * gain[:, k : k + block].astype(jnp.float32)).astype(jnp.bfloat16)

    def project(u, n, last, action):
        rows = n * UNIT
        load_turn(u, n).wait()
        t, r = raw[:rows, :], pltpu.roll(raw[:rows, :], HEAD // 2, 1)
        low = lax.broadcasted_iota(jnp.int32, t.shape, 1) < HEAD // 2
        cs[0, :rows, :HEAD] = jnp.where(low, t, r)
        cs[0, :rows, HEAD:] = jnp.where(low, -r, t)

        def store(t, count):
            for i in range(count):
                h = jnp.maximum(2 * t + i, 0)
                m = h // heads
                row = jnp.where(m == 0, q_row, jnp.where(m == 1, u * UNIT, v_row))
                which = jnp.where(m == 2, 1, 0)
                wide = fresh[t % 2, :rows, i * HEAD : (i + 1) * HEAD].astype(jnp.float32)
                turned = wide * cs[which, :rows, :HEAD] + pltpu.roll(wide, HEAD // 2, 1) * cs[which, :rows, HEAD:]
                big[pl.ds(pl.multiple_of(row, UNIT), rows), pl.ds(pl.multiple_of((h % heads) * HEAD, HEAD), HEAD)] = turned.astype(jnp.bfloat16)

        def body(t, _):
            @pl.when((t < tiles - 1) | jnp.logical_not(last))
            def _():
                start_tile((t + 1) % tiles, (t + 1) % 2)
            action(t)
            wait_tile(t % 2)
            store(t + 1 - 2, 2)
            fresh[t % 2, :rows, :] = dot(a[:rows, :], ring[t % 2]).astype(jnp.bfloat16)
        lax.fori_loop(0, tiles, body, None)
        store(tiles - 1, 1)
        for h in range(heads):
            vc[h, :HEAD, span(u, n)] = big[v_row : v_row + rows, h * HEAD : (h + 1) * HEAD].T

    def attend(u, mine):
        top[...] = jnp.full(top.shape, NEG, jnp.float32)
        mix[...] = jnp.zeros(mix.shape, jnp.float32)

        def block(j, masked):
            scores = [dot(big[span(j), h * HEAD : (h + 1) * HEAD], big[mine, h * HEAD : (h + 1) * HEAD], 1, 1) for h in range(heads)]
            weights, keeps = [], []
            for h, s in enumerate(scores):
                if masked:
                    seen = lax.broadcasted_iota(jnp.int32, s.shape, 1) >= lax.broadcasted_iota(jnp.int32, s.shape, 0)
                    s = jnp.where(seen, s, HIDDEN)
                old = top[h : h + 1, :]
                new = jnp.maximum(old, s.max(axis=0, keepdims=True))
                top[h : h + 1, :] = new
                weights.append(jnp.exp2((s - new) * scale).astype(jnp.bfloat16))
                keeps.append(jnp.exp2((old - new) * scale))
            for h, (p, keep) in enumerate(zip(weights, keeps)):
                mix[h] = mix[h] * keep + dot(vc[h, :, span(j)], p)

        lax.fori_loop(0, u, lambda j, _: block(j, False), None)
        block(u, True)
        for h in range(heads):
            big[mine, h * HEAD : (h + 1) * HEAD] = (mix[h, :HEAD, :] * (1 / mix[h, HEAD : HEAD + 1, :])).T.astype(jnp.bfloat16)

    def out_project(u, count, turn_no, last, ahead, action, ready):
        rows = count * UNIT
        at = pl.ds(pl.multiple_of(u % 2 * UNIT, UNIT), rows) if count == 1 else slice(None)

        def step(n):
            @pl.when((n < 6) | jnp.logical_not(last))
            def _():
                load_wo(piece((n + 2) % 8), (8 * turn_no + n + 2) % 3).start()
            action(n)

        def term(n):
            slot = (8 * turn_no + n) % 3
            load_wo(0, slot).wait()
            norm(*ahead(n))
            return dot(big[q_row : q_row + rows, :], wt[slot])

        def others(first, j):
            def body(i, _):
                n = first + i
                step(n)
                send0[at, cols(i)] = term(n).astype(jnp.bfloat16)
                for v in range(count):
                    s0(u + v, j + i).start()
            lax.fori_loop(0, 2, body, None)

        def ours(first, j, put):
            def body(i, _):
                n = first + i
                step(n)
                for v in range(count):
                    s0(u + v, j + i).wait()
                got = term(n)
                for v in range(count):
                    put(u + v, i, got[v * UNIT : (v + 1) * UNIT] + r0[(u + v) % 2, :, cols(j + i)].astype(jnp.float32))
                if put is send:
                    for v in range(count):
                        s1(u + v, i).start()
            lax.fori_loop(0, 2, body, None)

        def send(w, i, total):
            send1[w % 2, :, cols(i)] = total.astype(jnp.bfloat16)

        def keep(w, i, total):
            kept[w % 2, :, cols(i)] = total

        others(0, 0)
        ready()
        ours(2, 0, send)
        others(4, 2)
        ours(6, 2, keep)

    def at_steps(*plan):
        def action(t):
            for when, guard, f, u in plan:
                @pl.when((t == when) & guard)
                def _():
                    f(u)
        return action

    yes = jnp.bool_(True)
    quarter = UNIT // 2

    def load_quarter(i):
        at = slice(i * quarter, (i + 1) * quarter)
        return pltpu.make_async_copy(x.at[at, :], a.at[at, :], first_sem.at[i])

    for i in range(4):
        load_quarter(i).start()
    load_turn(0, 2).start()
    cs[1, :, :HEAD] = jnp.ones((cs.shape[1], HEAD), jnp.float32)
    cs[1, :, HEAD:] = jnp.zeros((cs.shape[1], HEAD), jnp.float32)
    vc[:, HEAD:, :] = jnp.ones((heads, vc.shape[1] - HEAD, vc.shape[2]), jnp.bfloat16)
    start_tile(jnp.int32(0), 0)
    for i in range(4):
        load_quarter(i).wait()

        def first_norm(k, _):
            norm(i * quarter + k * 32, 32)
        lax.fori_loop(0, quarter // 32, first_norm, None)
    load_wo(piece(0), 0).start()
    load_wo(piece(1), 1).start()

    def pair(p, _):
        u = 2 * p
        last, rest = p == PAIRS - 1, p >= 1
        b, c = u - 2, u - 1
        project(u, 2, last, at_steps((0, rest, after_near, b), (3, rest, after_near, c), (8, rest, after_far, b), (12, rest, after_far, c)))

        @pl.when(jnp.logical_not(last))
        def _():
            load_x(u + 2, 2).start()
            load_turn(u + 2, 2).start()

        def half(v, _):
            attend(u + v, pl.ds(pl.multiple_of(q_row + v * UNIT, UNIT), UNIT))
        lax.fori_loop(0, 2, half, None)

        @pl.when(jnp.logical_not(last))
        def _():
            load_x(u + 2, 2).wait()

        @pl.when(rest)
        def _():
            for w in (b, c):
                gather_own(w, G0_OWN, mate).wait_recv()
        out_project(u, 2, p, last, lambda n: (n * 64, 64), at_steps((0, rest, after_g2, b), (2, p >= 2, after_g1, b - 2), (4, rest, after_g2, c), (7, p >= 2, after_g1, c - 2)),
                    lambda: pl.when(rest)(lambda: pl.semaphore_wait(read_sem, 2)))
    lax.fori_loop(0, PAIRS, pair, None)

    b, c = UNITS - 2, UNITS - 1
    after_near(b)
    after_near(c)
    after_far(b)
    after_g1(c - 2)
    after_g1(b - 2)
    after_far(c)
    after_g2(b)
    after_g2(c)
    after_g1(c)
    after_g1(b)
    pl.semaphore_wait(read_sem, 2)
    for w in (b, c):
        gather_own(w, G0_OWN, mate).wait_recv()
    lax.fori_loop(0, UNITS, lambda u, _: finish(u), None)


def solution(mesh):
    def step(x, gain, wq, wk, wv, wo):
        tokens, depth = x.shape
        width = wq.shape[1]
        heads = width // HEAD
        anywhere = pl.BlockSpec(memory_space=pl.ANY)
        vmem = pl.BlockSpec(memory_space=pltpu.VMEM)
        bf16, f32 = jnp.bfloat16, jnp.float32
        return pl.pallas_call(
            kernel,
            out_shape=jax.ShapeDtypeStruct((tokens, depth), bf16),
            in_specs=[anywhere, vmem] + [anywhere] * 5,
            out_specs=anywhere,
            scratch_shapes=[
                pltpu.VMEM((2 * UNIT, depth), bf16),
                pltpu.VMEM((2, depth, TILE), bf16),
                pltpu.VMEM((tokens + 4 * UNIT, width), bf16),
                pltpu.VMEM((heads, HEAD + 16, tokens), bf16),
                pltpu.VMEM((3, width, width), bf16),
                pltpu.VMEM((2, 2 * UNIT, TILE), bf16),
                pltpu.VMEM((2 * UNIT, 2 * width), bf16),
                pltpu.VMEM((2, UNIT, 2 * width), bf16),
                pltpu.VMEM((2, UNIT, 2 * width), f32),
                pltpu.VMEM((2, UNIT, width), bf16),
                pltpu.VMEM((2, UNIT, width), bf16),
                pltpu.VMEM((2, UNIT, 4 * width), bf16),
                pltpu.VMEM((2, UNIT, 2 * width), bf16),
                pltpu.VMEM((2, UNIT, width), bf16),
                pltpu.VMEM((heads, UNIT), f32),
                pltpu.VMEM((heads, HEAD + 16, UNIT), f32),
                pltpu.VMEM((2 * UNIT, HEAD), f32),
                pltpu.VMEM((2, 2 * UNIT, 2 * HEAD), f32),
                pltpu.SemaphoreType.DMA((UNITS, COPIES)),
                pltpu.SemaphoreType.DMA((UNITS, COPIES)),
                pltpu.SemaphoreType.DMA((2,)),
                pltpu.SemaphoreType.DMA((3,)),
                pltpu.SemaphoreType.DMA,
                pltpu.SemaphoreType.DMA,
                pltpu.SemaphoreType.DMA((2,)),
                pltpu.SemaphoreType.REGULAR,
                pltpu.SemaphoreType.DMA((4,)),
            ],
            compiler_params=pltpu.CompilerParams(collective_id=0, has_side_effects=True, vmem_limit_bytes=67043328),
            name="layer",
        )(x, gain[None], wq, wk, wv, wo, jnp.asarray(table(tokens, HEAD // 2)))

    tokens, columns = P("dp", None), P(None, "tp")
    return jax.shard_map(
        step,
        mesh=mesh,
        in_specs=(tokens, P(None), columns, columns, columns, P("tp", None)),
        out_specs=tokens,
        check_vma=False,
    )
```
